32 devices in a mesh: unit: 2 (over core), zero: 4 (over z), model: 4 (over y, x).
Axes of the slice: x: 2, y: 2, z: 4, core: 2. Of those that a mesh axis runs over, the one named last changes fastest.
Arguments:
- first_query: float32 [16384, 8192], P(('unit', 'zero'), 'model'), parts along dimension 0, may hold values from -0.09375 to 0.09375
- second_query: float32 [16384, 8192], P(('unit', 'zero'), 'model'), parts along dimension 0, may hold values from -0.0625 to 0.0625
- first_key: float32 [16384, 1024], P(('unit', 'zero'), 'model'), parts along dimension 0, may hold values from -0.09375 to 0.09375
- second_key: float32 [16384, 1024], P(('unit', 'zero'), 'model'), parts along dimension 0, may hold values from -0.0625 to 0.0625
- first_value: float32 [16384, 1024], P(('unit', 'zero'), 'model'), parts along dimension 0, may hold values from -0.09375 to 0.09375
- second_value: float32 [16384, 1024], P(('unit', 'zero'), 'model'), parts along dimension 0, may hold values from -0.0625 to 0.0625
- mix_share: float32 [16384], P(('unit', 'zero')), parts along dimension 0, may hold values from 0.2 to 0.8
- norm_train: float32 [16384], P(('unit', 'zero', 'model')), parts along dimension 0, may hold values from 0.25 to 1.75
- norm_step: float32 [16384], P(('unit', 'zero', 'model')), parts along dimension 0, may hold values from -0.3 to 0.3
Outputs:
- serve_query: bfloat16 [16384, 8192], P('unit', 'model'), parts along dimension 0
- serve_key: bfloat16 [16384, 1024], P('unit', 'model'), parts along dimension 0
- serve_value: bfloat16 [16384, 1024], P('unit', 'model'), parts along dimension 0
- factor_query: float32 [16384], P(('unit', 'model')), parts along dimension 0
- factor_key: float32 [2048], P(('unit', 'model')), parts along dimension 0
- factor_value: float32 [2048], P(('unit', 'model')), parts along dimension 0
- serve_norm: bfloat16 [16384], P('unit'), parts along dimension 0
The draws below stay inside these ranges and needn't reach their ends.
There are 2 independent parts, one for each index of `unit`. The reference program is written for one: setup_inputs(seed, part) draws one part's arguments, and reference() takes and returns one part's arrays. A program takes and returns all parts, laid end to end along the dimension named above; each array names one. Nothing has to cross between parts.
All inputs are finite; a program needn't handle non-finite values.
Results may differ from the reference program's by a relative error of at most 0.0004.
Values may be sent and summed in bfloat16 or wider, within the bound.
A program may use at most 192 MiB of HBM per device.

```python
import jax
import jax.numpy as jnp
from jax import lax

D_MODEL = 8192
Q_DIM = 8192
KV_DIM = 1024


def with_spikes(values, rng, source, target, shards_of, factor):
    owner, partner = [(jnp.arange(values.shape[dim]) // (values.shape[dim] // shards_of)).reshape([-1 if axis == dim else 1 for axis in range(values.ndim)]) for dim in (source, target)]
    chosen = jax.random.permutation(rng, shards_of)[partner]
    strong = (owner == chosen) | (owner == (partner + shards_of // 2) % shards_of)
    return jnp.where(strong, factor * values, values)


def level_of(rng, shape, cuts, smallest, high):
    def one(axis_at, blocks):
        draws = jax.random.uniform(jax.random.fold_in(jax.random.fold_in(rng, 6), axis_at), (blocks,), jnp.float32, smallest / len(cuts), high / len(cuts))
        return jnp.repeat(jnp.exp(draws), shape[axis_at] // blocks).reshape((-1,) + (1,) * (len(shape) - axis_at - 1))

    loudness = one(*cuts[0])
    for cut in cuts[1:]:
        loudness = loudness * one(*cut)
    return loudness


def normal_values(stream_key, extent, deviation, reach, cuts=(), dtype=jnp.bfloat16):
    entries = deviation * jax.random.normal(stream_key, extent, jnp.float32)
    if cuts:
        entries = entries * level_of(stream_key, extent, cuts, -0.22, 0.18)
    return jnp.clip(entries, -reach, reach).astype(dtype)


def noise_with(own_key, extent, deviation, most, cuts, heavy, held_as=jnp.bfloat16):
    values = deviation * jax.random.normal(own_key, extent, jnp.float32)
    if cuts:
        values = values * level_of(own_key, extent, cuts, -0.22, 0.18)
    return jnp.clip(with_spikes(values, jax.random.fold_in(own_key, 3), *heavy), -most, most).astype(held_as)


def setup_inputs(seed: int = 0, part: int = 0) -> dict:
    key_list = jax.random.split(jax.random.key(seed), 10)
    own_keys = jax.random.split(jax.random.fold_in(key_list[9], part), 10)
    return {
        "first_query": noise_with(own_keys[0], (D_MODEL, Q_DIM), D_MODEL ** -0.5, 0.09375, ((0, 4), (1, 4)), (0, 1, 4, 2.0), jnp.float32),
        "second_query": normal_values(own_keys[1], (D_MODEL, Q_DIM), D_MODEL ** -0.5, 0.0625, ((0, 4), (1, 4)), jnp.float32),
        "first_key": noise_with(own_keys[2], (D_MODEL, KV_DIM), D_MODEL ** -0.5, 0.09375, ((0, 4), (1, 4)), (0, 1, 4, 2.0), jnp.float32),
        "second_key": normal_values(own_keys[3], (D_MODEL, KV_DIM), D_MODEL ** -0.5, 0.0625, ((0, 4), (1, 4)), jnp.float32),
        "first_value": noise_with(own_keys[4], (D_MODEL, KV_DIM), D_MODEL ** -0.5, 0.09375, ((0, 4), (1, 4)), (0, 1, 4, 2.0), jnp.float32),
        "second_value": normal_values(own_keys[5], (D_MODEL, KV_DIM), D_MODEL ** -0.5, 0.0625, ((0, 4), (1, 4)), jnp.float32),
        "mix_share": jnp.clip(0.2 + 0.6 * jax.random.uniform(own_keys[6], (D_MODEL,), jnp.float32) ** level_of(own_keys[6], (D_MODEL,), ((0, 4),), -0.2, 0.2), 0.2, 0.8),
        "norm_train": jnp.clip(1.0 + 0.15 * jax.random.normal(own_keys[7], (D_MODEL,), jnp.float32), 0.25, 1.75),
        "norm_step": jnp.clip(jax.random.uniform(own_keys[8], (D_MODEL,), jnp.float32, -0.3, 0.3) * level_of(own_keys[8], (D_MODEL,), ((0, 16),), -0.4, 0.0), -0.3, 0.3),
    }


def reference(first_query, second_query, first_key, second_key, first_value, second_value, mix_share, norm_train, norm_step):
    fresh_query = mix_share[:, None] * first_query + (1.0 - mix_share[:, None]) * second_query
    fresh_key = mix_share[:, None] * first_key + (1.0 - mix_share[:, None]) * second_key
    fresh_value = mix_share[:, None] * first_value + (1.0 - mix_share[:, None]) * second_value
    factor_query = jnp.sqrt(lax.optimization_barrier(jnp.sum(fresh_query * fresh_query, axis=0)))
    serve_query = (fresh_query / factor_query).astype(jnp.bfloat16)
    factor_key = jnp.sqrt(lax.optimization_barrier(jnp.sum(fresh_key * fresh_key, axis=0)))
    serve_key = (fresh_key / factor_key).astype(jnp.bfloat16)
    factor_value = jnp.sqrt(lax.optimization_barrier(jnp.sum(fresh_value * fresh_value, axis=0)))
    serve_value = (fresh_value / factor_value).astype(jnp.bfloat16)
    serve_norm = (norm_train + norm_step).astype(jnp.bfloat16)
    return (serve_query, serve_key, serve_value, factor_query, factor_key, factor_value, serve_norm)
```

```python
import functools

import jax
import jax.numpy as jnp
from jax import lax
from jax.experimental import pallas as pl
from jax.experimental.pallas import tpu as pltpu
from jax.sharding import PartitionSpec as P

MESH = pl.DeviceIdType.MESH
PIECES = 4


def exchange_kernel(n_zero, n_model, part_ref, norm_ref, total_ref, gain_ref, held, sent, got, sent_norm, got_norm, own):
    z, m = lax.axis_index("zero"), lax.axis_index("model")
    count = n_zero * n_model
    me = z * n_model + m
    barrier = pltpu.get_barrier_semaphore()

    def place(k):
        peer = lax.rem(me + k, count)
        return {"zero": peer // n_model, "model": lax.rem(peer, n_model)}

    for k in range(1, count):
        pl.semaphore_signal(barrier, inc=1, device_id=place(k), device_id_type=MESH)
    pl.semaphore_wait(barrier, count - 1)

    copies = []
    for k in range(1, n_zero):
        copies.append(
            pltpu.make_async_remote_copy(
                src_ref=part_ref,
                dst_ref=held.at[z],
                send_sem=sent.at[k],
                recv_sem=got.at[k],
                device_id={"zero": lax.rem(z + k, n_zero)},
                device_id_type=MESH,
            )
        )
    for k in range(1, count):
        copies.append(
            pltpu.make_async_remote_copy(
                src_ref=norm_ref,
                dst_ref=gain_ref.at[me],
                send_sem=sent_norm.at[k],
                recv_sem=got_norm.at[k],
                device_id=place(k),
                device_id_type=MESH,
            )
        )
    for copy in copies:
        copy.start()
    mine = [
        pltpu.make_async_copy(part_ref, held.at[z], own.at[0]),
        pltpu.make_async_copy(norm_ref, gain_ref.at[me], own.at[1]),
    ]
    for copy in mine:
        copy.start()
    for copy in mine + copies:
        copy.wait()
    total = held[0]
    for k in range(1, n_zero):
        total = total + held[k]
    total_ref[...] = total


def exchange(part, norm, n_zero, n_model):
    count = n_zero * n_model
    vmem = pl.BlockSpec(memory_space=pltpu.VMEM)
    return pl.pallas_call(
        functools.partial(exchange_kernel, n_zero, n_model),
        out_shape=(
            jax.ShapeDtypeStruct(part.shape, part.dtype),
            jax.ShapeDtypeStruct((count,) + norm.shape, norm.dtype),
        ),
        in_specs=[vmem, vmem],
        out_specs=(vmem, vmem),
        scratch_shapes=[
            pltpu.VMEM((n_zero,) + part.shape, part.dtype),
            pltpu.SemaphoreType.DMA((n_zero,)),
            pltpu.SemaphoreType.DMA((n_zero,)),
            pltpu.SemaphoreType.DMA((count,)),
            pltpu.SemaphoreType.DMA((count,)),
            pltpu.SemaphoreType.DMA((2,)),
        ],
        compiler_params=pltpu.CompilerParams(collective_id=0, has_side_effects=True),
        name="exchange",
    )(part, norm)


def on_device(
    n_zero,
    n_model,
    first_query,
    second_query,
    first_key,
    second_key,
    first_value,
    second_value,
    mix_share,
    norm_train,
    norm_step,
):
    pairs = ((first_query, second_query), (first_key, second_key), (first_value, second_value))
    share = mix_share[:, None]
    rows = share.shape[0]
    z = lax.axis_index("zero")

    def fresh_of(pair, low, high):
        first, second = pair[0][low:high], pair[1][low:high]
        return share[low:high] * first + (1.0 - share[low:high]) * second

    sums = []
    for pair in pairs:
        fresh = fresh_of(pair, 0, rows)
        sums.append(jnp.sum(fresh * fresh, axis=0))
    widths = [part.shape[0] for part in sums]
    total, gain = exchange(
        jnp.concatenate(sums)[None, :],
        (norm_train + norm_step).astype(jnp.bfloat16)[None, :],
        n_zero,
        n_model,
    )
    factor = jnp.sqrt(total[0])
    factors = jnp.split(factor, [widths[0], widths[0] + widths[1]])

    step = rows // PIECES
    pieces = [(1, 0, rows)]
    pieces += [(0, low, low + step) for low in range(0, rows, step)]
    pieces += [(2, 0, rows)]
    ring = [(k, (k + 1) % n_zero) for k in range(n_zero)]
    blocks = [
        (fresh_of(pairs[which], low, high) / factors[which]).astype(jnp.bfloat16)
        for which, low, high in pieces
    ]
    blocks[1:] = [lax.optimization_barrier(block) for block in blocks[1:]]
    serve = [
        jnp.zeros((n_zero * rows, width), jnp.bfloat16) for width in widths
    ]
    for hop in range(n_zero):
        owner = lax.rem(z + n_zero - hop, n_zero)
        moved = []
        for (which, low, high), block in zip(pieces, blocks):
            if hop < n_zero - 1:
                moved.append(lax.ppermute(block, "zero", ring))
            serve[which] = lax.dynamic_update_slice(
                serve[which], block, (owner * rows + low, jnp.zeros_like(owner))
            )
        blocks = moved
    return (*serve, *factors, gain.reshape(-1))


def solution(mesh):
    in_specs = (
        P(("unit", "zero"), "model"),
        P(("unit", "zero"), "model"),
        P(("unit", "zero"), "model"),
        P(("unit", "zero"), "model"),
        P(("unit", "zero"), "model"),
        P(("unit", "zero"), "model"),
        P(("unit", "zero")),
        P(("unit", "zero", "model")),
        P(("unit", "zero", "model")),
    )
    out_specs = (
        P("unit", "model"),
        P("unit", "model"),
        P("unit", "model"),
        P(("unit", "model")),
        P(("unit", "model")),
        P(("unit", "model")),
        P("unit"),
    )
    return jax.shard_map(
        functools.partial(on_device, mesh.shape["zero"], mesh.shape["model"]),
        mesh=mesh,
        in_specs=in_specs,
        out_specs=out_specs,
        check_vma=False,
    )
```

```python
import functools

import jax
import jax.numpy as jnp
from jax import lax
from jax.experimental import pallas as pl
from jax.experimental.pallas import tpu as pltpu
from jax.sharding import PartitionSpec as P


MESH = pl.DeviceIdType.MESH
PIECES = 4


def exchange_kernel(n_zero, n_model, part_ref, norm_ref, total_ref, gain_ref, held, sent, got, sent_norm, got_norm, own):
    z, m = lax.axis_index("zero"), lax.axis_index("model")
    count = n_zero * n_model
    me = z * n_model + m
    barrier = pltpu.get_barrier_semaphore()

    def place(k):
        peer = lax.rem(me + k, count)
        return {"zero": peer // n_model, "model": lax.rem(peer, n_model)}

    for k in range(1, count):
        pl.semaphore_signal(barrier, inc=1, device_id=place(k), device_id_type=MESH)
    pl.semaphore_wait(barrier, count - 1)

    copies = []
    for k in range(1, n_zero):
        copies.append(
            pltpu.make_async_remote_copy(
                src_ref=part_ref,
                dst_ref=held.at[z],
                send_sem=sent.at[k],
                recv_sem=got.at[k],
                device_id={"zero": lax.rem(z + k, n_zero)},
                device_id_type=MESH,
            )
        )
    for k in range(1, count):
        copies.append(
            pltpu.make_async_remote_copy(
                src_ref=norm_ref,
                dst_ref=gain_ref.at[me],
                send_sem=sent_norm.at[k],
                recv_sem=got_norm.at[k],
                device_id=place(k),
                device_id_type=MESH,
            )
        )
    for copy in copies:
        copy.start()
    mine = [
        pltpu.make_async_copy(part_ref, held.at[z], own.at[0]),
        pltpu.make_async_copy(norm_ref, gain_ref.at[me], own.at[1]),
    ]
    for copy in mine:
        copy.start()
    for copy in mine + copies:
        copy.wait()
    total = held[0]
    for k in range(1, n_zero):
        total = total + held[k]
    total_ref[...] = total


def exchange(part, norm, n_zero, n_model):
    count = n_zero * n_model
    vmem = pl.BlockSpec(memory_space=pltpu.VMEM)
    return pl.pallas_call(
        functools.partial(exchange_kernel, n_zero, n_model),
        out_shape=(
            jax.ShapeDtypeStruct(part.shape, part.dtype),
            jax.ShapeDtypeStruct((count,) + norm.shape, norm.dtype),
        ),
        in_specs=[vmem, vmem],
        out_specs=(vmem, vmem),
        scratch_shapes=[
            pltpu.VMEM((n_zero,) + part.shape, part.dtype),
            pltpu.SemaphoreType.DMA((n_zero,)),
            pltpu.SemaphoreType.DMA((n_zero,)),
            pltpu.SemaphoreType.DMA((count,)),
            pltpu.SemaphoreType.DMA((count,)),
            pltpu.SemaphoreType.DMA((2,)),
        ],
        compiler_params=pltpu.CompilerParams(collective_id=0, has_side_effects=True),
        name="exchange",
    )(part, norm)


def merge(
    n_zero,
    n_model,
    first_query,
    second_query,
    first_key,
    second_key,
    first_value,
    second_value,
    mix_share,
    norm_train,
    norm_step,
):
    pairs = ((first_query, second_query), (first_key, second_key), (first_value, second_value))
    share = mix_share[:, None]
    rows = share.shape[0]
    z = lax.axis_index("zero")

    def fresh_of(pair, low, high):
        first, second = pair[0][low:high], pair[1][low:high]
        return share[low:high] * first + (1.0 - share[low:high]) * second

    def sums_of(pair):
        fresh = fresh_of(pair, 0, rows)
        return jnp.sum(fresh * fresh, axis=0)

    def narrow(which, low, high, after=None):
        scale = factors[which]
        if after is not None:
            scale, _ = lax.optimization_barrier((scale, after))
        block = (fresh_of(pairs[which], low, high) / scale).astype(jnp.bfloat16)
        return lax.optimization_barrier(block)

    ring = [[(k, (k + shift) % n_zero) for k in range(n_zero)] for shift in range(n_zero)]
    total, gain = exchange(
        sums_of(pairs[1])[None, :],
        (norm_train + norm_step).astype(jnp.bfloat16)[None, :],
        n_zero,
        n_model,
    )
    factors = [None, jnp.sqrt(total[0]), None]
    key_block = narrow(1, 0, rows)
    key_moved = lax.ppermute(key_block, "zero", ring[1])
    first_query, second_query, first_value, second_value, _ = lax.optimization_barrier(
        (first_query, second_query, first_value, second_value, key_block)
    )
    pairs = ((first_query, second_query), pairs[1], (first_value, second_value))
    part = jnp.concatenate([sums_of(pairs[0]), sums_of(pairs[2])])
    parts = [part] + [lax.ppermute(part, "zero", ring[shift]) for shift in range(1, n_zero)]
    stack = jnp.stack(parts)
    total = sum(
        lax.dynamic_index_in_dim(stack, lax.rem(z + n_zero - k, n_zero), 0, keepdims=False)
        for k in range(n_zero)
    )
    factor = jnp.sqrt(total)
    width = first_query.shape[1]
    factors[0], factors[2] = factor[:width], factor[width:]

    step = rows // PIECES
    pieces = [(1, 0, rows), (2, 0, rows)]
    pieces += [(0, low, low + step) for low in range(0, rows, step)]
    blocks = [key_block]
    for k, piece in enumerate(pieces[1:], 1):
        blocks.append(narrow(*piece, after=blocks[-1]))
    widths = [pair[0].shape[1] for pair in pairs]
    serve = [
        jnp.zeros((n_zero * rows, width), jnp.bfloat16) for width in widths
    ]
    for hop in range(n_zero):
        owner = lax.rem(z + n_zero - hop, n_zero)
        moved = []
        for k, ((which, low, high), block) in enumerate(zip(pieces, blocks)):
            if hop == 0 and k == 0:
                moved.append(key_moved)
            elif hop < n_zero - 1:
                moved.append(lax.ppermute(block, "zero", ring[1]))
            serve[which] = lax.dynamic_update_slice(
                serve[which], block, (owner * rows + low, jnp.zeros_like(owner))
            )
        blocks = moved
    return (*serve, *factors, gain.reshape(-1))


def solution(mesh):
    in_specs = (
        P(("unit", "zero"), "model"),
        P(("unit", "zero"), "model"),
        P(("unit", "zero"), "model"),
        P(("unit", "zero"), "model"),
        P(("unit", "zero"), "model"),
        P(("unit", "zero"), "model"),
        P(("unit", "zero")),
        P(("unit", "zero", "model")),
        P(("unit", "zero", "model")),
    )
    out_specs = (
        P("unit", "model"),
        P("unit", "model"),
        P("unit", "model"),
        P(("unit", "model")),
        P(("unit", "model")),
        P(("unit", "model")),
        P("unit"),
    )
    return jax.shard_map(
        functools.partial(merge, mesh.shape["zero"], mesh.shape["model"]),
        mesh=mesh,
        in_specs=in_specs,
        out_specs=out_specs,
        check_vma=False,
    )
```
